16 devices in a mesh: rep: 4 (over y, z, core), dp: 4 (over x).
Axes of the slice: x: 4, y: 2, z: 1, core: 2. Of those that a mesh axis runs over, the one named last changes fastest.
The devices are a block of a 4x4x8 slice.
Arguments:
- x: bfloat16 [16, 2048, 896], P(('rep', 'dp')), parts along dimension 0
- dy: bfloat16 [16, 2048, 896], P(('rep', 'dp')), parts along dimension 0
- wq: bfloat16 [2, 896, 1024], P(None, 'dp')
- wk: bfloat16 [2, 896, 512], P(None, 'dp')
- wv: bfloat16 [2, 896, 512], P(None, 'dp')
- wo: bfloat16 [2, 1024, 896], P(None, 'dp')
- w_gate: bfloat16 [2, 896, 3584], P(None, 'dp')
- w_up: bfloat16 [2, 896, 3584], P(None, 'dp')
- w_down: bfloat16 [2, 3584, 896], P(None, 'dp')
- m_wq: float32 [2, 896, 1024], P(None, 'dp')
- m_wk: float32 [2, 896, 512], P(None, 'dp')
- m_wv: float32 [2, 896, 512], P(None, 'dp')
- m_wo: float32 [2, 1024, 896], P(None, 'dp')
- m_w_gate: float32 [2, 896, 3584], P(None, 'dp')
- m_w_up: float32 [2, 896, 3584], P(None, 'dp')
- m_w_down: float32 [2, 3584, 896], P(None, 'dp')
- v_wq: float32 [2, 896, 1024], P(None, 'dp')
- v_wk: float32 [2, 896, 512], P(None, 'dp')
- v_wv: float32 [2, 896, 512], P(None, 'dp')
- v_wo: float32 [2, 1024, 896], P(None, 'dp')
- v_w_gate: float32 [2, 896, 3584], P(None, 'dp')
- v_w_up: float32 [2, 896, 3584], P(None, 'dp')
- v_w_down: float32 [2, 3584, 896], P(None, 'dp')
Outputs:
- output 1: bfloat16 [8, 896, 1024], P('rep', 'dp'), parts along dimension 0
- output 2: bfloat16 [8, 896, 512], P('rep', 'dp'), parts along dimension 0
- output 3: bfloat16 [8, 896, 512], P('rep', 'dp'), parts along dimension 0
- output 4: bfloat16 [8, 1024, 896], P('rep', 'dp'), parts along dimension 0
- output 5: bfloat16 [8, 896, 3584], P('rep', 'dp'), parts along dimension 0
- output 6: bfloat16 [8, 896, 3584], P('rep', 'dp'), parts along dimension 0
- output 7: bfloat16 [8, 3584, 896], P('rep', 'dp'), parts along dimension 0
- output 8: float32 [8, 896, 1024], P('rep', 'dp'), parts along dimension 0
- output 9: float32 [8, 896, 512], P('rep', 'dp'), parts along dimension 0
- output 10: float32 [8, 896, 512], P('rep', 'dp'), parts along dimension 0
- output 11: float32 [8, 1024, 896], P('rep', 'dp'), parts along dimension 0
- output 12: float32 [8, 896, 3584], P('rep', 'dp'), parts along dimension 0
- output 13: float32 [8, 896, 3584], P('rep', 'dp'), parts along dimension 0
- output 14: float32 [8, 3584, 896], P('rep', 'dp'), parts along dimension 0
- output 15: float32 [8, 896, 1024], P('rep', 'dp'), parts along dimension 0
- output 16: float32 [8, 896, 512], P('rep', 'dp'), parts along dimension 0
- output 17: float32 [8, 896, 512], P('rep', 'dp'), parts along dimension 0
- output 18: float32 [8, 1024, 896], P('rep', 'dp'), parts along dimension 0
- output 19: float32 [8, 896, 3584], P('rep', 'dp'), parts along dimension 0
- output 20: float32 [8, 896, 3584], P('rep', 'dp'), parts along dimension 0
- output 21: float32 [8, 3584, 896], P('rep', 'dp'), parts along dimension 0
There are 4 independent parts. The reference program is written for one: setup_inputs(seed, part) draws one part's arguments, and reference() takes and returns one part's arrays. A program takes and returns all parts, laid end to end along the dimension named above; an argument that names none is the same for every part.
All inputs are finite; a program needn't handle non-finite values.
Results may differ from the reference program's by a relative error of at most 0.024.
Values are sent between devices in bfloat16 or wider.
A program may use at most 768 MiB of HBM per device.

```python
import jax
import jax.numpy as jnp
from jax import lax

SEQUENCES = 4
TOKENS = 2048
D = 896
HEADS = 4
KV_HEADS = 2
HEAD = 256
FF = 3584
LAYERS = 2
THETA = 10000
NAMES = ("wq", "wk", "wv", "wo", "w_gate", "w_up", "w_down")
SHAPES = {
    "wq": (LAYERS, D, HEADS * HEAD),
    "wk": (LAYERS, D, KV_HEADS * HEAD),
    "wv": (LAYERS, D, KV_HEADS * HEAD),
    "wo": (LAYERS, HEADS * HEAD, D),
    "w_gate": (LAYERS, D, FF),
    "w_up": (LAYERS, D, FF),
    "w_down": (LAYERS, FF, D),
}


def bump(key, n, height):
    away = (jnp.arange(n, dtype=jnp.int32) - jax.random.randint(key, (), 0, n, jnp.int32)) % n
    return jnp.where(away < n // 8, height, 1.0)


def together(key, own, strength):
    shared = jax.random.normal(key, own.shape[1:], jnp.float32)
    return (own + strength * shared) * lax.rsqrt(1 + strength * strength)


def setup_inputs(seed: int = 0, part: int = 0) -> dict:
    kx, kdy, ka, kb, kz, kf, kh, kl, *keys = jax.random.split(jax.random.key(seed), 8 + 3 * len(NAMES))
    kx, kdy, ka, kb = (jax.random.fold_in(k, part) for k in (kx, kdy, ka, kb))
    kw, km, kv = (keys[i::3] for i in range(3))
    shape = (SEQUENCES, TOKENS, D)
    much_x, much_dy = jax.random.uniform(kz, (2,), jnp.float32, 0.0, 1.0)
    loud = 2.0 ** jax.random.uniform(jax.random.fold_in(kz, 1), (), jnp.float32, -1.0, 2.0)
    layers = 2.0 ** jax.random.uniform(kl, (LAYERS, 1, 1), jnp.float32, -1.0, 1.0)
    times = {"wq": 1.0, "wk": 1.0, "wv": 2.0, "wo": layers, "w_gate": 1.0, "w_up": bump(kh, FF, 4.0), "w_down": layers}
    x = together(ka, jax.random.normal(kx, shape, jnp.float32), much_x) * bump(kf, D, 4.0)
    dy = together(kb, jax.random.normal(kdy, shape, jnp.float32), much_dy)
    drawn = {"x": x.astype(jnp.bfloat16), "dy": (loud * dy * (SEQUENCES * TOKENS) ** -0.5).astype(jnp.bfloat16)}
    for key, name in zip(kw, NAMES, strict=True):
        drawn[name] = (jax.random.normal(key, SHAPES[name], jnp.float32) * SHAPES[name][1] ** -0.5 * times[name]).astype(jnp.bfloat16)
    for key, name in zip(km, NAMES, strict=True):
        drawn[f"m_{name}"] = 0.1 * jax.random.normal(key, SHAPES[name], jnp.float32)
    for key, name in zip(kv, NAMES, strict=True):
        drawn[f"v_{name}"] = jax.random.uniform(key, SHAPES[name], jnp.float32, 0.02, 0.06)
    return drawn


def matmul(a, w):
    return jnp.dot(a, w, preferred_element_type=jnp.float32).astype(jnp.bfloat16)


def normed(h):
    wide = h.astype(jnp.float32)
    scale = lax.rsqrt(jnp.mean(wide**2, -1, keepdims=True) + 1e-6)
    return (wide * scale).astype(jnp.bfloat16)


def turned(t, theta):
    half = t.shape[-1] // 2
    angle = jnp.arange(t.shape[0], dtype=jnp.float32)[:, None] * theta ** (-jnp.arange(half, dtype=jnp.float32) / half)
    cos, sin = jnp.cos(angle)[:, None], jnp.sin(angle)[:, None]
    a, b = t[..., :half].astype(jnp.float32), t[..., half:].astype(jnp.float32)
    return jnp.concatenate([a * cos - b * sin, b * cos + a * sin], -1).astype(jnp.bfloat16)


def seen_by(q, k, v):
    tokens, kv = q.shape[0], k.shape[1]
    q = q.reshape(tokens, kv, -1, q.shape[-1])
    scores = jnp.einsum("tgsd,ugd->gstu", q.astype(jnp.float32), k.astype(jnp.float32)) * q.shape[-1] ** -0.5
    place = jnp.arange(tokens)
    weights = jax.nn.softmax(jnp.where(place[:, None] >= place, scores, -jnp.inf), -1).astype(jnp.bfloat16)
    return jnp.einsum("gstu,ugd->tgsd", weights.astype(jnp.float32), v.astype(jnp.float32)).astype(jnp.bfloat16).reshape(tokens, -1)


def layer(h, w):
    a = normed(h)
    q, k = (turned(matmul(a, w[name]).reshape(h.shape[0], -1, HEAD), THETA) for name in ("wq", "wk"))
    h = h + matmul(seen_by(q, k, matmul(a, w["wv"]).reshape(h.shape[0], -1, HEAD)), w["wo"])
    b = normed(h)
    gate = jnp.dot(b, w["w_gate"], preferred_element_type=jnp.float32)
    up = jnp.dot(b, w["w_up"], preferred_element_type=jnp.float32)
    return h + matmul((jax.nn.silu(gate) * up).astype(jnp.bfloat16), w["w_down"])


def adamw(w, m, v, g):
    m = 0.9 * m + 0.1 * g
    v = 0.95 * v + 0.05 * g * g
    step = m * lax.rsqrt(v + 1e-8) + 0.1 * w
    return (w - 0.02 * step).astype(jnp.bfloat16), m, v


def clipped(gradients, sum_of_squares, count):
    factor = jnp.minimum(1.0, 0.5 * lax.rsqrt(sum_of_squares / count + 1e-30))
    return [g * factor for g in gradients]


def stack(weights, h):
    return lax.scan(lambda h, w: (layer(h, w), None), h, weights)[0]


def reference(x, dy, wq, wk, wv, wo, w_gate, w_up, w_down, m_wq, m_wk, m_wv, m_wo, m_w_gate, m_w_up, m_w_down, v_wq, v_wk, v_wv, v_wo, v_w_gate, v_w_up, v_w_down):
    weights = dict(zip(NAMES, (wq, wk, wv, wo, w_gate, w_up, w_down), strict=True))

    def take(so_far, sequence):
        h, by_y = sequence
        _, back = jax.vjp(stack, weights, h)
        by_weights, by_h = back(by_y)
        return jax.tree.map(lambda total, term: total + term.astype(jnp.float32), so_far, by_weights), by_h

    none_yet = {name: jnp.zeros(w.shape, jnp.float32) for name, w in weights.items()}
    by_weights, by_x = lax.scan(take, none_yet, (x, dy))
    gradients = [by_weights[name].astype(jnp.bfloat16).astype(jnp.float32) for name in NAMES]
    gradients = clipped(gradients, sum(jnp.sum(g * g) for g in gradients), sum(g.size for g in gradients))
    first = (m_wq, m_wk, m_wv, m_wo, m_w_gate, m_w_up, m_w_down)
    second = (v_wq, v_wk, v_wv, v_wo, v_w_gate, v_w_up, v_w_down)
    new = [adamw(weights[name].astype(jnp.float32), m, v, g) for name, m, v, g in zip(NAMES, first, second, gradients, strict=True)]
    return tuple(one[which] for which in range(3) for one in new)
```

```python
import functools

import jax
import jax.numpy as jnp
from jax import lax
from jax.experimental import pallas as pl
from jax.experimental.pallas import tpu as pltpu
from jax.sharding import PartitionSpec as P

NEG = -1e30
HIDDEN = 2 * NEG
LOG2E = 1.4426950408889634
VMEM = 56 * 2**20
STRIP = 512


def _fit(size, want, unit=128):
    return max(n for n in range(unit, max(min(want, size), unit) + 1, unit) if size % n == 0)


def _dot(a, b, ca, cb):
    return lax.dot_general(a, b, (((ca,), (cb,)), ((), ())), preferred_element_type=jnp.float32)


def _seen(iq, bq, bk):
    first = iq * bq
    return lax.div(first + 1, bk), lax.div(first + bq - 1 + bk, bk)


def _gap(bk, cols, bq):
    return lax.rem(lax.broadcasted_iota(jnp.int32, (bk, cols), 1), bq) - lax.broadcasted_iota(jnp.int32, (bk, cols), 0)


def _row(ref, i):
    return jnp.concatenate([ref[0, i, n : n + 1, :] for n in range(ref.shape[2])], axis=1)


def _forward(q_ref, k_ref, v_ref, o_ref, lse_ref, top_s, mix_s, gap_s, *, scale, bq, bk):
    kb, g, d = q_ref.shape[1], q_ref.shape[2], q_ref.shape[4]
    low = k_ref.dtype
    cols = g * bq
    iq = pl.program_id(2)
    e = scale * LOG2E
    wide = _fit(cols, STRIP)
    pieces = [(i, at) for i in range(kb) for at in range(0, cols, wide)]
    gap_s[...] = _gap(bk, cols, bq)
    top_s[...] = jnp.full_like(top_s, NEG)
    mix_s[...] = jnp.zeros_like(mix_s)
    ones = jnp.ones((8, bk), low)

    def block(j, masked):
        here = pl.ds(j * bk, bk)
        scores = [_dot(k_ref[0, i, here, :], q_ref[0, i].reshape(cols, d)[at : at + wide, :], 1, 1) for i, at in pieces]
        ok = gap_s[...] >= j * bk - iq * bq if masked else None
        weights, keeps = [], []
        for (i, at), s in zip(pieces, scores):
            if masked:
                s = jnp.where(ok[:, at : at + wide], s, HIDDEN)
            old = top_s[i : i + 1, at : at + wide]
            top = jnp.maximum(old, s.max(axis=0, keepdims=True))
            top_s[i : i + 1, at : at + wide] = top
            weights.append(jnp.exp2((s - top) * e).astype(low))
            keeps.append(jnp.exp2((old - top) * e))
        for (i, at), p, keep in zip(pieces, weights, keeps):
            values = jnp.concatenate([v_ref[0, i, here, :].T, ones], axis=0)
            mix_s[i, :, at : at + wide] = mix_s[i, :, at : at + wide] * keep + _dot(values, p, 1, 0)

    whole, last = _seen(iq, bq, bk)
    lax.fori_loop(0, whole, lambda j, _: block(j, False), None)
    lax.fori_loop(whole, last, lambda j, _: block(j, True), None)
    for i in range(kb):
        total = mix_s[i, d : d + 1, :]
        o_ref[0, i] = (mix_s[i, :d, :] * (1 / total)).T.reshape(g, bq, d).astype(o_ref.dtype)
        lse = top_s[i : i + 1, :] * scale + jnp.log(total)
        for n in range(g):
            lse_ref[0, i, n : n + 1, :] = lse[:, n * bq : (n + 1) * bq]


def attend(q, k, v):
    b, h, s, d = q.shape
    kv = k.shape[1]
    g = h // kv
    bq, bk = _fit(s, 8 * STRIP // h), _fit(s, STRIP)
    queries = pl.BlockSpec((1, kv, g, bq, d), lambda ib, ih, iq: (ib, ih, 0, iq, 0))
    keys = pl.BlockSpec((1, kv, s, d), lambda ib, ih, iq: (ib, ih, 0, 0))
    stats = pl.BlockSpec((1, kv, g, bq), lambda ib, ih, iq: (ib, ih, 0, iq))
    out, lse = pl.pallas_call(
        functools.partial(_forward, scale=d**-0.5, bq=bq, bk=bk),
        grid=(b, 1, s // bq),
        in_specs=[queries, keys, keys],
        out_specs=[queries, stats],
        scratch_shapes=[pltpu.VMEM((kv, g * bq), jnp.float32), pltpu.VMEM((kv, d + 8, g * bq), jnp.float32), pltpu.VMEM((bk, g * bq), jnp.int32)],
        out_shape=[jax.ShapeDtypeStruct((b, kv, g, s, d), q.dtype), jax.ShapeDtypeStruct((b, kv, g, s), jnp.float32)],
        compiler_params=pltpu.CompilerParams(dimension_semantics=("parallel",) * 3, vmem_limit_bytes=VMEM),
        cost_estimate=pl.CostEstimate(flops=4 * b * h * s * s * d, transcendentals=b * h * s * s, bytes_accessed=6 * q.size),
        name="attend",
    )(q.reshape(b, kv, g, s, d), k, v)
    return out.reshape(b, h, s, d), lse.reshape(b, h, s)


def row_dot(d_out, out):
    return (d_out.astype(jnp.float32) * out.astype(jnp.float32)).sum(-1)


def _backward(q_ref, k_ref, v_ref, do_ref, lse_ref, delta_ref, dq_ref, dk_ref, dv_ref, dq_s, dk_s, dv_s, gap_s, *, scale, bq, bk):
    kb, g, d = q_ref.shape[1], q_ref.shape[2], q_ref.shape[4]
    low = q_ref.dtype
    cols = g * bq
    iq = pl.program_id(2)
    e = scale * LOG2E
    wide = _fit(cols, STRIP)
    pieces = [(i, at) for i in range(kb) for at in range(0, cols, wide)]

    @pl.when(iq == 0)
    def _():
        gap_s[...] = _gap(bk, cols, bq)
        dk_s[...] = jnp.zeros_like(dk_s)
        dv_s[...] = jnp.zeros_like(dv_s)

    dq_s[...] = jnp.zeros_like(dq_s)
    lses = [_row(lse_ref, i) * LOG2E for i in range(kb)]
    deltas = [_row(delta_ref, i) for i in range(kb)]

    def block(j, masked):
        here = pl.ds(j * bk, bk)
        qs = [q_ref[0, i].reshape(cols, d)[at : at + wide, :] for i, at in pieces]
        dos = [do_ref[0, i].reshape(cols, d)[at : at + wide, :] for i, at in pieces]
        scores = [_dot(k_ref[0, i, here, :], x, 1, 1) for (i, _), x in zip(pieces, qs)]
        dps = [_dot(v_ref[0, i, here, :], x, 1, 1) for (i, _), x in zip(pieces, dos)]
        ok = gap_s[...] >= j * bk - iq * bq if masked else None
        for n, (i, at) in enumerate(pieces):
            p = jnp.exp2(scores[n] * e - lses[i][:, at : at + wide])
            if masked:
                p = jnp.where(ok[:, at : at + wide], p, 0.0)
            ds = (p * (dps[n] - deltas[i][:, at : at + wide])).astype(low)
            dv_s[i, here, :] += _dot(p.astype(low), dos[n], 1, 0)
            dk_s[i, here, :] += _dot(ds, qs[n], 1, 0)
            dq_s[i, :, at : at + wide] += _dot(k_ref[0, i, here, :].T, ds, 1, 0)

    whole, last = _seen(iq, bq, bk)
    lax.fori_loop(0, whole, lambda j, _: block(j, False), None)
    lax.fori_loop(whole, last, lambda j, _: block(j, True), None)
    for i in range(kb):
        dq_ref[0, i] = (dq_s[i] * scale).T.reshape(g, bq, d).astype(dq_ref.dtype)

    @pl.when(iq == pl.num_programs(2) - 1)
    def _():
        dk_ref[0] = (dk_s[...] * scale).astype(dk_ref.dtype)
        dv_ref[0] = dv_s[...].astype(dv_ref.dtype)


def attend_bwd(q, k, v, d_out, lse, delta):
    b, h, s, d = q.shape
    kv = k.shape[1]
    g = h // kv
    bq, bk = _fit(s, 4 * STRIP // h), _fit(s, STRIP)
    queries = pl.BlockSpec((1, kv, g, bq, d), lambda ib, ih, iq: (ib, ih, 0, iq, 0))
    keys = pl.BlockSpec((1, kv, s, d), lambda ib, ih, iq: (ib, ih, 0, 0))
    stats = pl.BlockSpec((1, kv, g, bq), lambda ib, ih, iq: (ib, ih, 0, iq))
    dq, dk, dv = pl.pallas_call(
        functools.partial(_backward, scale=d**-0.5, bq=bq, bk=bk),
        grid=(b, 1, s // bq),
        in_specs=[queries, keys, keys, queries, stats, stats],
        out_specs=[queries, keys, keys],
        scratch_shapes=[pltpu.VMEM((kv, d, g * bq), jnp.float32), pltpu.VMEM((kv, s, d), jnp.float32), pltpu.VMEM((kv, s, d), jnp.float32),
                        pltpu.VMEM((bk, g * bq), jnp.int32)],
        out_shape=[jax.ShapeDtypeStruct((b, kv, g, s, d), q.dtype), jax.ShapeDtypeStruct(k.shape, q.dtype), jax.ShapeDtypeStruct(v.shape, q.dtype)],
        compiler_params=pltpu.CompilerParams(dimension_semantics=("parallel", "parallel", "arbitrary"), vmem_limit_bytes=VMEM),
        cost_estimate=pl.CostEstimate(flops=10 * b * h * s * s * d, transcendentals=b * h * s * s, bytes_accessed=12 * q.size),
        name="attend_bwd",
    )(q.reshape(b, kv, g, s, d), k, v, d_out.reshape(b, kv, g, s, d), lse.reshape(b, kv, g, s), delta.reshape(b, kv, g, s))
    return dq.reshape(b, h, s, d), dk, dv


HEAD = 256
THETA = 10000


BF, F32 = jnp.bfloat16, jnp.float32
EPS = 1e-6


def _params(*semantics):
    return pltpu.CompilerParams(dimension_semantics=semantics, vmem_limit_bytes=VMEM)


def _work(flops, *arrays):
    return pl.CostEstimate(flops=flops, transcendentals=0, bytes_accessed=sum(a.size * a.dtype.itemsize for a in arrays))


def _like(shape, dtype=BF):
    return jax.ShapeDtypeStruct(shape, dtype)


def _scale(wide):
    return lax.rsqrt(jnp.mean(wide * wide, -1, keepdims=True) + EPS)


def _norm_back(wide, by_out):
    scale = _scale(wide)
    return by_out * scale - wide * (scale * scale * scale * jnp.mean(by_out * wide, -1, keepdims=True))


PART = 512


def _turned(t, cos, sin):
    half = t.shape[-1] // 2
    a, b = t[:, :half].astype(F32), t[:, half:].astype(F32)
    return jnp.concatenate([a * cos - b * sin, b * cos + a * sin], -1).astype(BF)


def _qkv_kernel(h_ref, w_ref, cos_ref, sin_ref, a_ref, q_ref, k_ref, v_ref, *, heads, kv):
    n = pl.program_id(0)
    tokens = h_ref.shape[0]
    parts = [slice(i, i + PART) for i in range(0, tokens, PART)]

    @pl.when(n == 0)
    def _():
        for here in parts:
            wide = h_ref[here, :].astype(F32)
            a_ref[here, :] = (wide * _scale(wide)).astype(BF)

    def put(ref, turn):
        made = [_dot(a_ref[here, :], w_ref[...], 1, 0).astype(BF) for here in parts]
        for here, t in zip(parts, made):
            ref[0, here, :] = _turned(t, cos_ref[here, :], sin_ref[here, :]) if turn else t

    pl.when(n < heads)(lambda: put(q_ref, True))
    pl.when((n >= heads) & (n < heads + kv))(lambda: put(k_ref, True))
    pl.when(n >= heads + kv)(lambda: put(v_ref, False))


def project(h, w, first, cos, sin, heads, kv):
    tokens, d = h.shape
    whole = lambda n: (0, 0)
    one = lambda first, count: (lambda n: (jnp.clip(n - first, 0, count - 1), 0, 0))
    return pl.pallas_call(
        functools.partial(_qkv_kernel, heads=heads, kv=kv),
        grid=(heads + 2 * kv,),
        in_specs=[pl.BlockSpec((tokens, d), whole), pl.BlockSpec((d, HEAD), lambda n: (0, first + n)), pl.BlockSpec(cos.shape, whole), pl.BlockSpec(sin.shape, whole)],
        out_specs=[pl.BlockSpec((tokens, d), whole), pl.BlockSpec((1, tokens, HEAD), one(0, heads)), pl.BlockSpec((1, tokens, HEAD), one(heads, kv)),
                   pl.BlockSpec((1, tokens, HEAD), one(heads + kv, kv))],
        out_shape=[_like((tokens, d)), _like((heads, tokens, HEAD)), _like((kv, tokens, HEAD)), _like((kv, tokens, HEAD))],
        compiler_params=_params("arbitrary"),
        cost_estimate=_work(2 * tokens * d * (heads + 2 * kv) * HEAD, h, h, h, h),
        name="project",
    )(h, w, cos, sin)


def _qkv_back_kernel(dq_ref, dk_ref, dv_ref, a_ref, w1_ref, w2_ref, cos_ref, sin_ref, h_ref, dh_ref, dx_ref, dw_ref, at_s, t_s, *, heads, kv):
    n = pl.program_id(0)
    tokens = a_ref.shape[0]
    parts = [slice(i, i + PART) for i in range(0, tokens, PART)]

    @pl.when(n == 0)
    def _():
        for here in parts:
            at_s[:, here] = a_ref[here, :].T

    def back(ref):
        for here in parts:
            t_s[n, here, :] = _turned(ref[0, here, :], cos_ref[here, :], -sin_ref[here, :])

    pl.when(n < heads)(lambda: back(dq_ref))
    pl.when((n >= heads) & (n < heads + kv))(lambda: back(dk_ref))

    @pl.when(n >= heads + kv)
    def _():
        t_s[n] = dv_ref[0]

    dw_ref[...] = _dot(at_s[...], t_s[n], 1, 0).astype(BF)

    @pl.when(n == pl.num_programs(0) - 1)
    def _():
        def finish(i, _):
            here = pl.ds(i * PART, PART)
            most = t_s.shape[0] // 2
            t1, t2 = (jnp.concatenate([t_s[one, here, :] for one in range(i, i + most)], axis=1) for i in (0, most))
            by_a = (_dot(t1, w1_ref[...], 1, 1) + _dot(t2, w2_ref[...], 1, 1)).astype(BF).astype(F32)
            by_h = _norm_back(h_ref[here, :].astype(F32), by_a).astype(BF)
            dx_ref[here, :] = (dh_ref[here, :].astype(F32) + by_h.astype(F32)).astype(BF)

        lax.fori_loop(0, tokens // PART, finish, None)


def project_back(dq, dk, dv, a, w, first, cos, sin, h, dh):
    heads, tokens, _ = dq.shape
    kv, d = dk.shape[0], a.shape[1]
    count = heads + 2 * kv
    part = count // 2
    whole = lambda n: (0, 0)
    one = lambda first, count: (lambda n: (jnp.clip(n - first, 0, count - 1), 0, 0))
    full = pl.BlockSpec((tokens, d), whole)
    return pl.pallas_call(
        functools.partial(_qkv_back_kernel, heads=heads, kv=kv),
        grid=(count,),
        in_specs=[pl.BlockSpec((1, tokens, HEAD), one(0, heads)), pl.BlockSpec((1, tokens, HEAD), one(heads, kv)),
                  pl.BlockSpec((1, tokens, HEAD), one(heads + kv, kv)), full, *(pl.BlockSpec((d, part * HEAD), lambda n, i=i: (0, first // part + i)) for i in range(2)),
                  pl.BlockSpec(cos.shape, whole), pl.BlockSpec(sin.shape, whole), full, full],
        out_specs=[full, pl.BlockSpec((d, HEAD), lambda n: (0, n))],
        out_shape=[_like((tokens, d)), _like((d, count * HEAD))],
        scratch_shapes=[pltpu.VMEM((d, tokens), BF), pltpu.VMEM((count, tokens, HEAD), BF)],
        compiler_params=_params("arbitrary"),
        cost_estimate=_work(4 * tokens * d * count * HEAD, dq, dk, dv, a, h, dh, h, h, h),
        name="project_back",
    )(dq, dk, dv, a, w, w, cos, sin, h, dh)


def _out_kernel(o_ref, w_ref, h_ref, h1_ref, b_ref):
    heads = o_ref.shape[0]
    o = jnp.concatenate([o_ref[n] for n in range(heads)], axis=1)
    new = (h_ref[...].astype(F32) + _dot(o, w_ref[...].reshape(o.shape[1], -1), 1, 0).astype(BF).astype(F32)).astype(BF)
    h1_ref[...] = new
    wide = new.astype(F32)
    b_ref[...] = (wide * _scale(wide)).astype(BF)


def out_project(o, w, layer, h):
    heads, tokens, _ = o.shape
    d, m = h.shape[1], 512
    row = pl.BlockSpec((m, d), lambda i: (i, 0))
    return pl.pallas_call(
        _out_kernel,
        grid=(tokens // m,),
        in_specs=[pl.BlockSpec((heads, m, HEAD), lambda i: (0, i, 0)), pl.BlockSpec((w.shape[0], None, *w.shape[2:]), lambda i: (0, layer, 0, 0)), row],
        out_specs=[row, row],
        out_shape=[_like(h.shape), _like(h.shape)],
        compiler_params=_params("arbitrary"),
        cost_estimate=_work(2 * tokens * heads * HEAD * d, o, w, h, h, h),
        name="out_project",
    )(o, w, h)


def _out_back_kernel(dh_ref, w_ref, o_ref, do_ref, dw_ref):
    w = w_ref[...].reshape(HEAD, -1)
    for i in range(0, dh_ref.shape[0], PART):
        do_ref[0, i : i + PART, :] = _dot(dh_ref[i : i + PART, :], w, 1, 1).astype(BF)
    dw_ref[...] = _dot(o_ref[0].T, dh_ref[...], 1, 0).astype(BF)


def out_back(dh, w, layer, o):
    heads, tokens, _ = o.shape
    d = dh.shape[1]
    head = pl.BlockSpec((1, tokens, HEAD), lambda n: (n, 0, 0))
    return pl.pallas_call(
        _out_back_kernel,
        grid=(heads,),
        in_specs=[pl.BlockSpec((tokens, d), lambda n: (0, 0)), pl.BlockSpec((w.shape[0] // heads, None, *w.shape[2:]), lambda n: (n, layer, 0, 0)), head],
        out_specs=[head, pl.BlockSpec((HEAD, d), lambda n: (n, 0))],
        out_shape=[_like(o.shape), _like((heads * HEAD, d))],
        compiler_params=_params("arbitrary"),
        cost_estimate=_work(4 * tokens * heads * HEAD * d, dh, w, o, o, w),
        name="out_back",
    )(dh, w, o)


def _gate_kernel(b_ref, wg_ref, wu_ref, kept_ref, act_ref):
    size = act_ref.shape[0]
    for i in range(0, size, PART):
        here = slice(i, i + PART)
        b = b_ref[pl.ds(pl.program_id(1) * size + i, PART), :]
        g, u = _dot(b, wg_ref[...], 1, 0), _dot(b, wu_ref[...], 1, 0)
        kept_ref[0, 0, here, :], kept_ref[1, 0, here, :] = g, u
        act_ref[here, :] = (g * jax.nn.sigmoid(g) * u).astype(BF)


TILE = 512


def gate_up(b, w, ff):
    tokens, d = b.shape
    n, m = ff // TILE, 2 * PART
    return pl.pallas_call(
        _gate_kernel,
        grid=(n, tokens // m),
        in_specs=[pl.BlockSpec((tokens, d), lambda j, i: (0, 0)), pl.BlockSpec((d, TILE), lambda j, i: (0, j)), pl.BlockSpec((d, TILE), lambda j, i: (0, n + j))],
        out_specs=[pl.BlockSpec((2, 1, m, TILE), lambda j, i: (0, j, i, 0)), pl.BlockSpec((m, TILE), lambda j, i: (i, j))],
        out_shape=[_like((2, n, tokens, TILE), F32), _like((tokens, n * TILE))],
        compiler_params=_params("arbitrary", "arbitrary"),
        cost_estimate=_work(4 * tokens * d * ff, b, w),
        name="gate_up",
    )(b, w, w)


def _down_kernel(act_ref, w_ref, h_ref, out_ref):
    out_ref[...] = (h_ref[...].astype(F32) + _dot(act_ref[...], w_ref[...], 1, 0).astype(BF).astype(F32)).astype(BF)


def down(act, w, h):
    tokens, d = h.shape
    m = 256
    row = pl.BlockSpec((m, d), lambda i: (i, 0))
    return pl.pallas_call(
        _down_kernel,
        grid=(tokens // m,),
        in_specs=[pl.BlockSpec((m, act.shape[1]), lambda i: (i, 0)), pl.BlockSpec(w.shape, lambda i: (0, 0)), row],
        out_specs=row,
        out_shape=_like(h.shape),
        compiler_params=_params("arbitrary"),
        cost_estimate=_work(2 * tokens * w.size, act, w, h, h),
        name="down",
    )(act, w, h)


def _ffn_mid_kernel(dh_ref, wd_ref, kept_ref, dgu_ref):
    m = pl.program_id(1)
    size, part = kept_ref.shape[2], PART // 2
    das = [_dot(dh_ref[pl.ds(m * size + i, part), :], wd_ref[...], 1, 1).astype(BF).astype(F32) for i in range(0, size, part)]
    for i, da in enumerate(das):
        rows = slice(i * part, (i + 1) * part)
        g, u = kept_ref[0, 0, rows, :], kept_ref[1, 0, rows, :]
        s = jax.nn.sigmoid(g)
        gs = g * s
        dgu_ref[0, 0, rows, :] = (da * u * (s + gs * (1 - s))).astype(BF)
        dgu_ref[1, 0, rows, :] = (da * gs).astype(BF)


def ffn_mid(dh, w_down, kept):
    tokens, d = dh.shape
    n, m = kept.shape[1], 2 * PART
    tile = pl.BlockSpec((2, 1, m, TILE), lambda j, i: (0, j, i, 0))
    return pl.pallas_call(
        _ffn_mid_kernel,
        grid=(n, tokens // m),
        in_specs=[pl.BlockSpec((tokens, d), lambda j, i: (0, 0)), pl.BlockSpec((TILE, d), lambda j, i: (j, 0)), tile],
        out_specs=tile,
        out_shape=_like(kept.shape),
        compiler_params=_params("arbitrary", "arbitrary"),
        cost_estimate=_work(2 * tokens * w_down.size, dh, kept, w_down),
        name="ffn_mid",
    )(dh, w_down, kept)


def _ffn_in_kernel(dgu_ref, w_ref, h_ref, dh_ref, dx_ref):
    n = dgu_ref.shape[1]
    both = jnp.concatenate([dgu_ref[i, j] for i in range(2) for j in range(n)], axis=1)
    by_b = _dot(both, w_ref[...], 1, 1).astype(BF).astype(F32)
    by_h = _norm_back(h_ref[...].astype(F32), by_b).astype(BF)
    dx_ref[...] = (dh_ref[...].astype(F32) + by_h.astype(F32)).astype(BF)


def ffn_in(dgu, w, h, dh):
    tokens, d = h.shape
    n, m = dgu.shape[1], PART // 2
    row = pl.BlockSpec((m, d), lambda i: (i, 0))
    return pl.pallas_call(
        _ffn_in_kernel,
        grid=(tokens // m,),
        in_specs=[pl.BlockSpec((2, n, m, TILE), lambda i: (0, 0, i, 0)), pl.BlockSpec((d, 2 * n * TILE), lambda i: (0, 0)), row, row],
        out_specs=row,
        out_shape=_like((tokens, d)),
        compiler_params=_params("arbitrary"),
        cost_estimate=_work(4 * tokens * d * n * TILE, dgu, w, h, dh),
        name="ffn_in",
    )(dgu, w, h, dh)


def _gate_weights_kernel(b_ref, d_ref, out_ref, bt_s):
    @pl.when(pl.program_id(0) == 0)
    def _():
        for i in range(0, b_ref.shape[0], PART):
            bt_s[:, i : i + PART] = b_ref[i : i + PART, :].T

    out_ref[...] = _dot(bt_s[...], d_ref[0, 0], 1, 0).astype(BF)


def gate_weights(b, dgu):
    tokens, d = b.shape
    n = dgu.shape[1]
    return pl.pallas_call(
        _gate_weights_kernel,
        grid=(2 * n,),
        in_specs=[pl.BlockSpec((tokens, d), lambda j: (0, 0)), pl.BlockSpec((1, 1, tokens, TILE), lambda j: (j // n, j % n, 0, 0))],
        out_specs=pl.BlockSpec((d, TILE), lambda j: (0, j)),
        out_shape=_like((d, 2 * n * TILE)),
        scratch_shapes=[pltpu.VMEM((d, tokens), BF)],
        compiler_params=_params("arbitrary"),
        cost_estimate=_work(2 * tokens * d * 2 * n * TILE, b, dgu),
        name="gate_weights",
    )(b, dgu)


def adamw(w, m, v, g):
    m = 0.9 * m + 0.1 * g
    v = 0.95 * v + 0.05 * g * g
    step = m * lax.rsqrt(v + 1e-8) + 0.1 * w
    return (w - 0.02 * step).astype(jnp.bfloat16), m, v


def clipped(gradients, sum_of_squares, count):
    factor = jnp.minimum(1.0, 0.5 * lax.rsqrt(sum_of_squares / count + 1e-30))
    return [g * factor for g in gradients]


CORES = 2


def solution(mesh):
    grid = mesh.devices
    split = jax.sharding.Mesh(grid.reshape(grid.shape[0] // CORES, CORES, grid.shape[1]), ("chip", "core", "dp"))

    def fetched(w):
        half = w.shape[0] // CORES
        mine = lax.dynamic_slice_in_dim(w, lax.axis_index("core") * half, half, 0)
        return lax.all_gather(mine, ("dp", "core"), axis=0, tiled=True)

    def scattered(g):
        return lax.psum_scatter(g, "dp", scatter_dimension=0, tiled=True)

    def passed_on(g):
        n = grid.shape[1]
        me, rows = lax.axis_index("dp"), g.shape[0] // n
        half = rows // 2
        right, left = ([(i, (i + way) % n) for i in range(n)] for way in (1, n - 1))

        def send(t, way):
            return lax.ppermute(t, "dp", way)

        def block(place, first, count):
            return lax.dynamic_slice_in_dim(g, lax.rem(me + place, n) * rows + first, count, 0)

        def add(a, b):
            return (a.astype(F32) + b.astype(F32)).astype(BF)

        top = send(block(n // 2, 0, half), right)
        low = send(block(n // 2, half, half), left)
        to_right = jnp.concatenate([add(block(1, 0, half), top), block(1, half, half)])
        to_left = jnp.concatenate([block(n - 1, 0, half), add(block(n - 1, half, half), low)])
        from_left = send(to_right, right)
        from_right = send(to_left, left)
        return (block(0, 0, rows).astype(F32) + from_left.astype(F32) + from_right.astype(F32)).astype(BF)

    def work(x, dy, *arrays):
        weights, m, v = (arrays[i : i + 7] for i in (0, 7, 14))
        wq, wk, wv, wo, w_gate, w_up, w_down = weights
        layers, kv, heads = wq.shape[0], wk.shape[2] // HEAD, wq.shape[2] // HEAD
        ff = w_gate.shape[2]
        h = x[0]
        half = HEAD // 2
        angle = jnp.arange(h.shape[0], dtype=F32)[:, None] * THETA ** (-jnp.arange(half, dtype=F32) / half)
        cos, sin = jnp.cos(angle), jnp.sin(angle)

        cut = lambda n: [jnp.concatenate([wq[n], wk[n], wv[n]], 1), jnp.concatenate([w_gate[n], w_up[n]], 1)]
        columns = [cut(n) for n in range(layers)]
        gates = 2 * ff // HEAD
        w_in, at = fetched(columns[0][0]), 0
        rows = wo.shape[1] // CORES
        mine = lax.dynamic_slice_in_dim(wo, lax.axis_index("core") * rows, rows, 1).reshape(-1, wo.shape[2])
        w_out = lax.all_gather(mine, ("dp", "core"), axis=0, tiled=True).reshape(-1, layers, rows, wo.shape[2])
        kept = []
        for n in range(layers):
            w_gu = fetched(jnp.concatenate([columns[n][1], columns[n + 1][0]], 1) if n + 1 < layers else columns[n][1])
            w_dn = fetched(w_down[n])
            a, q, k, val = project(h, w_in, at, cos, sin, heads, kv)
            out, lse = attend(q[None], k[None], val[None])
            h1, b = out_project(out[0], w_out, n, h)
            gu, act = gate_up(b, w_gu, ff)
            kept.append((w_in, at, w_gu, w_dn, h, a, q, k, val, out, lse, h1, b, gu, act))
            h = down(act, w_dn, h1)
            w_in, at = w_gu, gates

        dh, parts = dy[0], [{} for _ in range(layers)]
        nq, nk = wq.shape[2], wk.shape[2]
        for n in reversed(range(layers)):
            w_in, at, w_gu, w_dn, h, a, q, k, val, out, lse, h1, b, gu, act = kept[n]
            by_down = lax.dot_general(act, dh, (((0,), (0,)), ((), ())), preferred_element_type=F32).astype(BF)
            dh, by_down = lax.optimization_barrier((dh, by_down))
            parts[n]["down"] = scattered(by_down)
            dgu = ffn_mid(dh, w_dn, gu)
            by_gu = gate_weights(b, dgu)
            dh, by_gu = lax.optimization_barrier((dh, by_gu))
            parts[n]["gu"] = scattered(by_gu)
            dh = ffn_in(dgu, w_gu, h1, dh)
            do, by_out = out_back(dh, w_out, n, out[0])
            parts[n]["out"] = passed_on(by_out)
            delta = row_dot(do[None], out)
            dq, dk, dv = attend_bwd(q[None], k[None], val[None], do[None], lse, delta)
            dh, by_in = project_back(dq[0], dk[0], dv[0], a, w_in, at, cos, sin, h, dh)
            parts[n]["in"] = passed_on(by_in)
        mine = [[p["in"][:, :nq], p["in"][:, nq : nq + nk], p["in"][:, nq + nk :], p["out"], p["gu"][:, :ff], p["gu"][:, ff:], p["down"]] for p in parts]
        squares = sum(jnp.sum(jnp.square(g.astype(F32))) for p in parts for g in p.values())
        squares = lax.psum(squares, "dp")
        count = lax.psum(1, "dp") * sum(w.size for w in weights)
        gradients = [jnp.stack([mine[n][i] for n in range(layers)]).astype(F32) for i in range(7)]
        gradients = clipped(gradients, squares, count)
        new = [adamw(w.astype(F32), m, v, g) for w, m, v, g in zip(weights, m, v, gradients, strict=True)]
        return tuple(one[which] for which in range(3) for one in new)

    states, cut = P(("chip", "core", "dp"), None, None), P(None, "dp", None)
    return jax.shard_map(
        work,
        mesh=split,
        in_specs=(states, states) + (cut,) * 21,
        out_specs=(P(("chip", "core"), "dp", None),) * 21,
        check_vma=False,
    )
```
